16 devices in a mesh: dp: 2 (over y, z), tp: 8 (over x, core).
Axes of the slice: x: 4, y: 2, z: 1, core: 2. Of those that a mesh axis runs over, the one named last changes fastest.
The devices are a block of a 4x4x8 slice.
Arguments:
- hidden: bfloat16 [12, 384, 5120], P('dp', 'tp'), parts along dimension 0
- lengths: int32 [12], P('dp'), parts along dimension 0
- rope_cos: float32 [12, 384, 32], P('dp'), parts along dimension 0
- rope_sin: float32 [12, 384, 32], P('dp'), parts along dimension 0
- cache_lat: bfloat16 [12, 896, 512], P('dp'), parts along dimension 0
- cache_pe: bfloat16 [12, 896, 64], P('dp'), parts along dimension 0
- norm_in: float32 [5120], replicated
- w_dq: bfloat16 [5120, 1536], replicated
- norm_q: float32 [1536], replicated
- w_dkv: bfloat16 [5120, 576], replicated
- norm_kv: float32 [512], replicated
- w_uq: bfloat16 [1536, 128, 192], P(None, 'tp')
- w_uk: bfloat16 [512, 128, 128], P(None, 'tp')
- w_uv: bfloat16 [512, 128, 128], P(None, 'tp')
- w_out: bfloat16 [16384, 5120], P('tp')
Outputs:
- output 1: bfloat16 [12, 384, 5120], P('dp', 'tp'), parts along dimension 0
- output 2: bfloat16 [12, 896, 512], P('dp'), parts along dimension 0
- output 3: bfloat16 [12, 896, 64], P('dp'), parts along dimension 0
There are 2 independent parts. The reference program is written for one: setup_inputs(seed, part) draws one part's arguments, and reference() takes and returns one part's arrays. A program takes and returns all parts, laid end to end along the dimension named above; an argument that names none is the same for every part.
All inputs are finite; a program needn't handle non-finite values.
Results may differ from the reference program's by a relative error of at most 0.0145318.
Values are sent between devices in bfloat16 or wider.
A program may use at most 768 MiB of HBM per device.

```python
import jax
import jax.numpy as jnp
from jax import lax

MODEL_DIM = 5120
NUM_HEADS = 128
Q_RANK = 1536
KV_RANK = 512
NOPE_DIM = 128
ROPE_DIM = 64
VALUE_DIM = 128
SEQ_COUNT = 6
CHUNK_LEN = 384
PREFIX_MAX = 512
CACHE_LEN = 896

HEAD_BLOCK = min(8, NUM_HEADS)


def rms_norm(values, gain_vec):
    inv_rms = lax.rsqrt(jnp.mean(values * values, axis=-1, keepdims=True) + 1e-6)
    return values * inv_rms * gain_vec


def apply_rope(values, cos_tab, sin_tab):
    half_dim = values.shape[-1] // 2
    lower_half = values[..., :half_dim]
    upper_half = values[..., half_dim:]
    return jnp.concatenate([lower_half * cos_tab - upper_half * sin_tab, upper_half * cos_tab + lower_half * sin_tab], axis=-1)


def write_rows(old_rows, new_rows, start_row):
    zero_col = jnp.zeros((), start_row.dtype)
    return lax.dynamic_update_slice(old_rows, new_rows.astype(old_rows.dtype), (start_row, zero_col))


def rope_tables(lengths):
    positions = (lengths[:, None] + jnp.arange(CHUNK_LEN)[None, :]).astype(jnp.float32)
    inv_freq = 10000.0 ** (-2.0 * jnp.arange(ROPE_DIM // 2).astype(jnp.float32) / ROPE_DIM)
    angles = positions[:, :, None] * inv_freq[None, None, :]
    return jnp.cos(angles), jnp.sin(angles)


def normal_draw(key_in, array_shape, std_scale):
    return jax.random.normal(key_in, array_shape, jnp.float32) * std_scale


def setup_inputs(seed: int = 0, part: int = 0) -> dict:
    base_key = jax.random.key(seed)
    part_keys = jax.random.split(jax.random.fold_in(base_key, part), 5)
    weight_keys = jax.random.split(base_key, 9)
    draw_vals = jax.random.randint(part_keys[0], (SEQ_COUNT,), PREFIX_MAX // 4, PREFIX_MAX + 1)
    top_slot = jax.random.randint(part_keys[1], (), 0, SEQ_COUNT)
    lengths = jnp.where(jnp.arange(SEQ_COUNT) == top_slot, PREFIX_MAX, draw_vals).astype(jnp.int32)
    rope_cos, rope_sin = rope_tables(lengths)
    out_scale = (NUM_HEADS * VALUE_DIM) ** -0.5 * (CACHE_LEN / 4.0) ** 0.5
    return {
        "hidden": normal_draw(part_keys[2], (SEQ_COUNT, CHUNK_LEN, MODEL_DIM), 1.0).astype(jnp.bfloat16),
        "lengths": lengths,
        "rope_cos": rope_cos,
        "rope_sin": rope_sin,
        "cache_lat": normal_draw(part_keys[3], (SEQ_COUNT, CACHE_LEN, KV_RANK), 1.0).astype(jnp.bfloat16),
        "cache_pe": normal_draw(part_keys[4], (SEQ_COUNT, CACHE_LEN, ROPE_DIM), 1.0).astype(jnp.bfloat16),
        "norm_in": jax.random.uniform(weight_keys[0], (MODEL_DIM,), jnp.float32, 0.5, 1.5),
        "w_dq": normal_draw(weight_keys[1], (MODEL_DIM, Q_RANK), MODEL_DIM ** -0.5).astype(jnp.bfloat16),
        "norm_q": jax.random.uniform(weight_keys[2], (Q_RANK,), jnp.float32, 0.5, 1.5),
        "w_dkv": normal_draw(weight_keys[3], (MODEL_DIM, KV_RANK + ROPE_DIM), MODEL_DIM ** -0.5).astype(jnp.bfloat16),
        "norm_kv": jax.random.uniform(weight_keys[4], (KV_RANK,), jnp.float32, 0.5, 1.5),
        "w_uq": normal_draw(weight_keys[5], (Q_RANK, NUM_HEADS, NOPE_DIM + ROPE_DIM), Q_RANK ** -0.5).astype(jnp.bfloat16),
        "w_uk": normal_draw(weight_keys[6], (KV_RANK, NUM_HEADS, NOPE_DIM), KV_RANK ** -0.5).astype(jnp.bfloat16),
        "w_uv": normal_draw(weight_keys[7], (KV_RANK, NUM_HEADS, VALUE_DIM), KV_RANK ** -0.5).astype(jnp.bfloat16),
        "w_out": normal_draw(weight_keys[8], (NUM_HEADS * VALUE_DIM, MODEL_DIM), out_scale).astype(jnp.bfloat16),
    }


def reference(hidden, lengths, rope_cos, rope_sin, cache_lat, cache_pe, norm_in, w_dq, norm_q, w_dkv, norm_kv, w_uq, w_uk, w_uv, w_out):
    hidden_f = hidden.astype(jnp.float32)
    normed = rms_norm(hidden_f, norm_in).astype(jnp.bfloat16).reshape(SEQ_COUNT * CHUNK_LEN, MODEL_DIM)
    q_latent = rms_norm(jnp.dot(normed, w_dq, preferred_element_type=jnp.float32), norm_q).astype(jnp.bfloat16)
    kv_proj = jnp.dot(normed, w_dkv, preferred_element_type=jnp.float32).reshape(SEQ_COUNT, CHUNK_LEN, KV_RANK + ROPE_DIM)
    new_lat = rms_norm(kv_proj[..., :KV_RANK], norm_kv).astype(jnp.bfloat16)
    new_pe = apply_rope(kv_proj[..., KV_RANK:], rope_cos, rope_sin).astype(jnp.bfloat16)
    lat_all = jax.vmap(write_rows)(cache_lat, new_lat, lengths)
    pe_all = jax.vmap(write_rows)(cache_pe, new_pe, lengths)
    q_full = jnp.einsum("nc,chd->nhd", q_latent.astype(jnp.float32), w_uq.astype(jnp.float32)).reshape(SEQ_COUNT, CHUNK_LEN, NUM_HEADS, NOPE_DIM + ROPE_DIM)
    q_nope = q_full[..., :NOPE_DIM].astype(jnp.bfloat16)
    q_pe = apply_rope(q_full[..., NOPE_DIM:], rope_cos[:, :, None, :], rope_sin[:, :, None, :]).astype(jnp.bfloat16)
    block_count = NUM_HEADS // HEAD_BLOCK
    uk_blocks = w_uk.reshape(KV_RANK, block_count, HEAD_BLOCK, NOPE_DIM).transpose(1, 0, 2, 3)
    uv_blocks = w_uv.reshape(KV_RANK, block_count, HEAD_BLOCK, VALUE_DIM).transpose(1, 0, 2, 3)
    score_scale = (NOPE_DIM + ROPE_DIM) ** -0.5
    query_pos = jnp.arange(CHUNK_LEN)[:, None]
    key_pos = jnp.arange(CACHE_LEN)[None, :]

    def one_sequence(seq_args):
        qn_seq, qp_seq, lat_seq, pe_seq, length = seq_args
        visible = key_pos < length + query_pos + 1
        qn_blocks = qn_seq.reshape(CHUNK_LEN, block_count, HEAD_BLOCK, NOPE_DIM).transpose(1, 0, 2, 3)
        qp_blocks = qp_seq.reshape(CHUNK_LEN, block_count, HEAD_BLOCK, ROPE_DIM).transpose(1, 0, 2, 3)
        lat_f = lat_seq.astype(jnp.float32)
        pe_f = pe_seq.astype(jnp.float32)

        def one_block(blk_args):
            qn_blk, qp_blk, uk_blk, uv_blk = blk_args
            keys_nope = jnp.einsum("sc,chd->shd", lat_f, uk_blk.astype(jnp.float32)).astype(jnp.bfloat16)
            values_blk = jnp.einsum("sc,chv->shv", lat_f, uv_blk.astype(jnp.float32)).astype(jnp.bfloat16)
            scores = jnp.einsum("thd,shd->hts", qn_blk.astype(jnp.float32), keys_nope.astype(jnp.float32))
            scores = scores + jnp.einsum("thr,sr->hts", qp_blk.astype(jnp.float32), pe_f)
            scores = jnp.where(visible[None], scores * score_scale, -1e30)
            attn_probs = jax.nn.softmax(scores, axis=-1).astype(jnp.bfloat16)
            return jnp.einsum("hts,shv->thv", attn_probs.astype(jnp.float32), values_blk.astype(jnp.float32)).astype(jnp.bfloat16)

        out_blocks = lax.map(one_block, (qn_blocks, qp_blocks, uk_blocks, uv_blocks))
        return out_blocks.transpose(1, 0, 2, 3).reshape(CHUNK_LEN, NUM_HEADS * VALUE_DIM)

    attn_out = lax.map(one_sequence, (q_nope, q_pe, lat_all, pe_all, lengths))
    out_proj = jnp.dot(attn_out.reshape(SEQ_COUNT * CHUNK_LEN, NUM_HEADS * VALUE_DIM), w_out, preferred_element_type=jnp.float32)
    block_out = (out_proj.reshape(SEQ_COUNT, CHUNK_LEN, MODEL_DIM) + hidden_f).astype(jnp.bfloat16)
    return (block_out, lat_all, pe_all)
```

```python
import functools

import jax
import jax.numpy as jnp
from jax import lax
from jax.experimental import pallas as pl
from jax.experimental.pallas import tpu as pltpu
from jax.sharding import PartitionSpec as P

BF16 = jnp.bfloat16
F32 = jnp.float32
NEG = -1e30
LOG2E = 1.4426950408889634
EPS = 1e-6
QBLK = 128
CORES = 2
MAIN_ID = 0


def rms_norm(values, gain_vec):
    inv_rms = lax.rsqrt(jnp.mean(values * values, axis=-1, keepdims=True) + EPS)
    return values * inv_rms * gain_vec


def apply_rope(values, cos_tab, sin_tab):
    half_dim = values.shape[-1] // 2
    lower_half = values[..., :half_dim]
    upper_half = values[..., half_dim:]
    return jnp.concatenate([lower_half * cos_tab - upper_half * sin_tab, upper_half * cos_tab + lower_half * sin_tab], axis=-1)


def dot_nn(lhs, rhs):
    return lax.dot_general(lhs, rhs, (((1,), (0,)), ((), ())), preferred_element_type=F32)


def dot_nt(lhs, rhs):
    return lax.dot_general(lhs, rhs, (((1,), (1,)), ((), ())), preferred_element_type=F32)


def rope_pair(values, cos_tab, sin_tab, half_dim):
    lanes = values.shape[1]
    upper = pltpu.roll(values, lanes - half_dim, 1)
    lower = pltpu.roll(values, half_dim, 1)
    lane = lax.broadcasted_iota(jnp.int32, values.shape, 1)
    swapped = jnp.where(lane % (2 * half_dim) < half_dim, upper, lower)
    return values * cos_tab + swapped * sin_tab


class Dims:
    pass


def main_kernel(dm, len_ref, gath_ref, lat_ref, pe_old_ref, cos_ref, sin_ref, wuq_ref, wuk_ref, wuv_ref, wout_ref, hid_ref, out_ref,
                q_buf, lat_buf, pe_buf, cos_buf, sin_buf, wuq_buf, wuk_buf, wuv_buf, wout_buf,
                qcat, kcat, vcat, attn_buf, part_buf, xch_buf, sum_buf, hop_buf, dir_buf, fin_buf, hid_buf, y_buf,
                seq_sem, w_sem, wout_sem, hid_sem, y_sem,
                xch_send, xch_recv, hop_send, hop_recv, dir_send, dir_recv, fin_send, fin_recv,
                credit_pair, credit_left, credit_right):
    me = lax.axis_index("tp")
    chip = me // CORES
    core = me % CORES
    chips = dm.chips
    left_chip = (chip + chips - 1) % chips
    right_chip = (chip + 1) % chips
    partner = chip * CORES + (1 - core)
    left = left_chip * CORES + core
    right = right_chip * CORES + core

    barrier = pltpu.get_barrier_semaphore()
    for peer in (partner, left, right):
        pl.semaphore_signal(barrier, inc=1, device_id={"tp": peer})
    pl.semaphore_wait(barrier, 3)

    groups, gh = dm.groups, dm.group_heads
    chunks, cw, hw, tok = dm.chunks, dm.chunk_cols, dm.half_cols, dm.tok
    attn_ticks = dm.seqs * groups
    out_ticks = dm.seqs * chunks
    nope, rope, vdim, prefix, qlen = dm.nope, dm.rope, dm.vdim, dm.prefix, dm.qlen
    nslot = dm.ring_slots

    def seq_copies(b, slot):
        return (
            pltpu.make_async_copy(gath_ref.at[b, :, pl.ds(0, dm.q_rank)], q_buf.at[slot], seq_sem.at[slot, 0]),
            pltpu.make_async_copy(lat_ref.at[b, pl.ds(0, prefix)], lat_buf.at[slot, pl.ds(0, prefix)], seq_sem.at[slot, 1]),
            pltpu.make_async_copy(gath_ref.at[b, :, pl.ds(dm.q_rank, dm.kv_rank)], lat_buf.at[slot, pl.ds(prefix, qlen)], seq_sem.at[slot, 2]),
            pltpu.make_async_copy(pe_old_ref.at[b], pe_buf.at[slot, pl.ds(0, prefix)], seq_sem.at[slot, 3]),
            pltpu.make_async_copy(gath_ref.at[b, :, pl.ds(dm.q_rank + dm.kv_rank, 2 * rope)], pe_buf.at[slot, pl.ds(prefix, qlen)], seq_sem.at[slot, 4]),
            pltpu.make_async_copy(cos_ref.at[b], cos_buf.at[slot], seq_sem.at[slot, 5]),
            pltpu.make_async_copy(sin_ref.at[b], sin_buf.at[slot], seq_sem.at[slot, 6]),
        )

    def weight_copies(g, slot):
        return (
            pltpu.make_async_copy(wuq_ref.at[pl.ds(g * gh, gh), pl.ds(0, nope)], wuq_buf.at[slot, pl.ds(0, gh * nope)].reshape(gh, nope, dm.q_rank), w_sem.at[slot, 0]),
            pltpu.make_async_copy(wuq_ref.at[pl.ds(g * gh, gh), pl.ds(nope, rope)], wuq_buf.at[slot, pl.ds(gh * nope, gh * rope)].reshape(gh, rope, dm.q_rank), w_sem.at[slot, 1]),
            pltpu.make_async_copy(wuk_ref.at[:, pl.ds(g * gh * nope, gh * nope)], wuk_buf.at[slot], w_sem.at[slot, 2]),
            pltpu.make_async_copy(wuv_ref.at[:, pl.ds(g * gh * vdim, gh * vdim)], wuv_buf.at[slot], w_sem.at[slot, 3]),
        )

    def wout_copy(j, slot):
        return pltpu.make_async_copy(wout_ref.at[:, pl.ds((j % chunks) * cw, cw)], wout_buf.at[slot], wout_sem.at[slot])

    def hid_copy(j, slot):
        return pltpu.make_async_copy(hid_ref.at[j // chunks, :, pl.ds((j % chunks) * cw, cw)], hid_buf.at[slot], hid_sem.at[slot])

    def y_copy(j, slot):
        return pltpu.make_async_copy(y_buf.at[slot], out_ref.at[j // chunks, :, pl.ds((j % chunks) * cw, cw)], y_sem.at[slot])

    def xch_copy(j, t):
        slot = j % 2
        return pltpu.make_async_remote_copy(
            src_ref=part_buf.at[slot, pl.ds(pl.multiple_of((t * CORES + 1 - core) * tok, 8), tok)],
            dst_ref=xch_buf.at[slot, t],
            send_sem=xch_send.at[slot, t],
            recv_sem=xch_recv.at[slot, t],
            device_id={"tp": partner},
        )

    def toward(u):
        if u == 0:
            return (left, left_chip), (right, right_chip)
        return (right, right_chip), (left, left_chip)

    def hop_copy(j, u):
        (down, _), _ = toward(u)
        return pltpu.make_async_remote_copy(
            src_ref=sum_buf.at[j % nslot, (chip + 2) % chips, :, pl.ds(u * hw, hw)],
            dst_ref=hop_buf.at[j % nslot, u],
            send_sem=hop_send.at[j % nslot, u],
            recv_sem=hop_recv.at[j % nslot, u],
            device_id={"tp": down},
        )

    def dir_copy(j, u):
        _, (up, up_chip) = toward(u)
        return pltpu.make_async_remote_copy(
            src_ref=sum_buf.at[j % nslot, up_chip, :, pl.ds(u * hw, hw)],
            dst_ref=dir_buf.at[j % nslot, u],
            send_sem=dir_send.at[j % nslot, u],
            recv_sem=dir_recv.at[j % nslot, u],
            device_id={"tp": up},
        )

    def fin_copy(j, u):
        (down, down_chip), _ = toward(u)
        return pltpu.make_async_remote_copy(
            src_ref=sum_buf.at[j % nslot, down_chip, :, pl.ds(u * hw, hw)],
            dst_ref=fin_buf.at[j % nslot, u],
            send_sem=fin_send.at[j % nslot, u],
            recv_sem=fin_recv.at[j % nslot, u],
            device_id={"tp": down},
        )

    def attention(b, g, wslot):
        slot = b % 2
        q_lat = q_buf[slot]
        lane = lax.broadcasted_iota(jnp.int32, (qlen, 2 * rope), 1)
        q_pe = dot_nt(q_lat, wuq_buf[wslot, gh * nope:])
        for pair in range(gh // 2):
            rotated = rope_pair(q_pe[:, pair * 2 * rope:(pair + 1) * 2 * rope], cos_buf[slot], sin_buf[slot], rope // 2)
            qcat[2 * pair, :, nope:] = jnp.where(lane < rope, rotated, 0.0).astype(BF16)
            qcat[2 * pair + 1, :, nope:] = jnp.where(lane >= rope, rotated, 0.0).astype(BF16)
        q_nope = dot_nt(q_lat, wuq_buf[wslot, :gh * nope])
        for h in range(gh):
            qcat[h, :, :nope] = q_nope[:, h * nope:(h + 1) * nope].astype(BF16)
        keys = dot_nn(lat_buf[slot], wuk_buf[wslot])
        for h in range(gh):
            kcat[h, :, :nope] = keys[:, h * nope:(h + 1) * nope].astype(BF16)
        vcat[...] = dot_nn(lat_buf[slot], wuv_buf[wslot]).astype(BF16)

        length = len_ref[b]
        key_pos = lax.broadcasted_iota(jnp.int32, (1, prefix), 1)
        bias = jnp.where(key_pos < length, 0.0, NEG).astype(F32)
        row = lax.broadcasted_iota(jnp.int32, (QBLK, QBLK), 0)
        col = lax.broadcasted_iota(jnp.int32, (QBLK, QBLK), 1)
        causal = col <= row
        nblk = qlen // QBLK
        wide = prefix + (nblk - 1) * QBLK
        for h in range(gh):
            main = dot_nt(qcat[h], kcat[h, :wide])
            last = dot_nt(qcat[h, (nblk - 1) * QBLK:], kcat[h, wide:])
            for blk in range(nblk):
                rows = slice(blk * QBLK, (blk + 1) * QBLK)
                pieces = [main[rows, :prefix] + bias]
                if blk == nblk - 1:
                    pieces.append(main[rows, prefix:wide])
                    diag = last
                else:
                    if blk > 0:
                        pieces.append(main[rows, prefix:prefix + blk * QBLK])
                    diag = main[rows, prefix + blk * QBLK:prefix + (blk + 1) * QBLK]
                pieces.append(jnp.where(causal, diag, NEG))
                top = functools.reduce(jnp.maximum, [jnp.max(piece, axis=1, keepdims=True) for piece in pieces])
                total = None
                acc = None
                start = 0
                for piece in pieces:
                    prob = jnp.exp2((piece - top) * dm.exp_scale)
                    piece_sum = jnp.sum(prob, axis=1, keepdims=True)
                    width = piece.shape[1]
                    term = dot_nn(prob.astype(BF16), vcat[start:start + width, h * vdim:(h + 1) * vdim])
                    total = piece_sum if total is None else total + piece_sum
                    acc = term if acc is None else acc + term
                    start += width
                attn_buf[slot, rows, pl.ds(pl.multiple_of((g * gh + h) * vdim, 128), vdim)] = (acc / total).astype(BF16)

    for copy in seq_copies(0, 0) + weight_copies(0, 0):
        copy.start()

    def tick(i, carry):
        b = i // groups
        g = i % groups
        wslot = i % 2

        @pl.when(i + 1 < attn_ticks)
        def _():
            for copy in weight_copies((i + 1) % groups, (i + 1) % 2):
                copy.start()

        @pl.when(jnp.logical_and(g == 1, b + 1 < dm.seqs))
        def _():
            for copy in seq_copies(b + 1, (b + 1) % 2):
                copy.start()

        j_next = i + 1 - groups

        @pl.when(jnp.logical_and(j_next >= 0, j_next < out_ticks))
        def _():
            wout_copy(j_next, j_next % 2).start()

        j1 = i - groups - 1

        @pl.when(jnp.logical_and(j1 >= 0, j1 < out_ticks))
        def _():
            hid_copy(j1, j1 % nslot).start()
            for t in range(chips):
                xch_copy(j1, t).wait_recv()
            for off in (2, 1, 3, 0):
                t = (chip + off) % chips
                rows = pl.ds(pl.multiple_of((t * CORES + core) * tok, 8), tok)
                sum_buf[j1 % nslot, t] = part_buf[j1 % 2, rows] + xch_buf[j1 % 2, t]

            @pl.when(j1 + 2 < out_ticks)
            def _():
                pl.semaphore_signal(credit_pair, inc=1, device_id={"tp": partner})

            @pl.when(j1 >= nslot)
            def _():
                pl.semaphore_wait(credit_left, 1)
                pl.semaphore_wait(credit_right, 1)

            for u in range(2):
                hop_copy(j1, u).start()
            for u in range(2):
                dir_copy(j1, u).start()

        j2 = i - groups - 2

        @pl.when(jnp.logical_and(j2 >= 0, j2 < out_ticks))
        def _():
            for u in range(2):
                hop_copy(j2, u).wait_recv()
            for u in range(2):
                _, down_chip = toward(u)[0]
                cols = pl.ds(u * hw, hw)
                sum_buf[j2 % nslot, down_chip, :, cols] = sum_buf[j2 % nslot, down_chip, :, cols] + hop_buf[j2 % nslot, u]
            for u in range(2):
                fin_copy(j2, u).start()

        j3 = i - groups - 3

        @pl.when(jnp.logical_and(j3 >= 0, j3 < out_ticks))
        def _():
            s3 = j3 % nslot
            hid_copy(j3, s3).wait()

            @pl.when(j3 >= 2)
            def _():
                y_copy(j3 - 2, j3 % 2).wait()

            for u in range(2):
                dir_copy(j3, u).wait()
                fin_copy(j3, u).wait()
                hop_copy(j3, u).wait_send()
            for u in range(2):
                cols = pl.ds(u * hw, hw)
                total = sum_buf[s3, chip, :, cols] + dir_buf[s3, u] + fin_buf[s3, u]
                y_buf[j3 % 2, :, cols] = (total + hid_buf[s3, :, cols].astype(F32)).astype(BF16)

            @pl.when(j3 + nslot < out_ticks)
            def _():
                pl.semaphore_signal(credit_left, inc=1, device_id={"tp": right})
                pl.semaphore_signal(credit_right, inc=1, device_id={"tp": left})

            y_copy(j3, j3 % 2).start()

        j0 = i - groups

        @pl.when(jnp.logical_and(j0 >= 0, j0 < out_ticks))
        def _():
            pslot = j0 % 2

            @pl.when(j0 >= 2)
            def _():
                for t in range(chips):
                    xch_copy(j0 - 2, t).wait_send()

            wout_copy(j0, pslot).wait()
            part_buf[pslot] = dot_nn(attn_buf[(j0 // chunks) % 2], wout_buf[pslot])

            @pl.when(j0 >= 2)
            def _():
                pl.semaphore_wait(credit_pair, 1)

            for t in range(chips):
                xch_copy(j0, t).start()

        @pl.when(i < attn_ticks)
        def _():
            @pl.when(g == 0)
            def _():
                for copy in seq_copies(b, b % 2):
                    copy.wait()
                for h in range(gh):
                    kcat[h, :, nope:] = pe_buf[b % 2]

            for copy in weight_copies(g, wslot):
                copy.wait()
            attention(b, g, wslot)

        return carry

    lax.fori_loop(0, out_ticks + groups + 3, tick, 0)

    for j in (out_ticks - 2, out_ticks - 1):
        for t in range(chips):
            xch_copy(j, t).wait_send()
        y_copy(j, j % 2).wait()


def attention_block(lengths, gathered, cache_lat, pe_old, cos_tab, sin_tab, w_uq_t, w_uk, w_uv, w_out, hidden, tp):
    dm = Dims()
    dm.seqs, dm.tok, dm.model = hidden.shape
    heads, head_dim, dm.q_rank = w_uq_t.shape
    dm.kv_rank = w_uk.shape[0]
    dm.nope = w_uk.shape[1] // heads
    dm.vdim = w_uv.shape[1] // heads
    dm.rope = head_dim - dm.nope
    dm.qlen = gathered.shape[1]
    dm.prefix = cache_lat.shape[1] - dm.qlen
    dm.chips = tp // CORES
    dm.group_heads = 4
    dm.groups = heads // dm.group_heads
    dm.chunks = 4
    dm.chunk_cols = dm.model // dm.chunks
    dm.half_cols = dm.chunk_cols // 2
    dm.ring_slots = 4
    dm.exp_scale = head_dim ** -0.5 * LOG2E
    gh, keys, ns = dm.group_heads, dm.prefix + dm.qlen, dm.ring_slots
    assert dm.chips == 4 and dm.groups == dm.chunks

    def vmem(*shape, dtype=BF16):
        return pltpu.VMEM(shape, dtype)

    dma = pltpu.SemaphoreType.DMA
    scratch = [
        vmem(2, dm.qlen, dm.q_rank),
        vmem(2, keys, dm.kv_rank),
        vmem(2, keys, 2 * dm.rope),
        vmem(2, dm.qlen, 2 * dm.rope, dtype=F32),
        vmem(2, dm.qlen, 2 * dm.rope, dtype=F32),
        vmem(2, gh * head_dim, dm.q_rank),
        vmem(2, dm.kv_rank, gh * dm.nope),
        vmem(2, dm.kv_rank, gh * dm.vdim),
        vmem(2, heads * dm.vdim, dm.chunk_cols),
        vmem(gh, dm.qlen, dm.nope + 2 * dm.rope),
        vmem(gh, keys, dm.nope + 2 * dm.rope),
        vmem(keys, gh * dm.vdim),
        vmem(2, dm.qlen, heads * dm.vdim),
        vmem(2, dm.qlen, dm.chunk_cols, dtype=F32),
        vmem(2, dm.chips, dm.tok, dm.chunk_cols, dtype=F32),
        vmem(ns, dm.chips, dm.tok, dm.chunk_cols, dtype=F32),
        vmem(ns, 2, dm.tok, dm.half_cols, dtype=F32),
        vmem(ns, 2, dm.tok, dm.half_cols, dtype=F32),
        vmem(ns, 2, dm.tok, dm.half_cols, dtype=F32),
        vmem(ns, dm.tok, dm.chunk_cols),
        vmem(2, dm.tok, dm.chunk_cols),
        dma((2, 7)), dma((2, 4)), dma((2,)), dma((ns,)), dma((2,)),
        dma((2, dm.chips)), dma((2, dm.chips)),
        dma((ns, 2)), dma((ns, 2)), dma((ns, 2)), dma((ns, 2)), dma((ns, 2)), dma((ns, 2)),
        pltpu.SemaphoreType.REGULAR, pltpu.SemaphoreType.REGULAR, pltpu.SemaphoreType.REGULAR,
    ]
    hbm = pl.BlockSpec(memory_space=pl.ANY)
    return pl.pallas_call(
        functools.partial(main_kernel, dm),
        out_shape=jax.ShapeDtypeStruct(hidden.shape, BF16),
        in_specs=[pl.BlockSpec(memory_space=pltpu.SMEM)] + [hbm] * 10,
        out_specs=hbm,
        scratch_shapes=scratch,
        compiler_params=pltpu.CompilerParams(collective_id=MAIN_ID, has_side_effects=True, vmem_limit_bytes=66_000_000),
        name="attend_project",
    )(lengths, gathered, cache_lat, pe_old, cos_tab, sin_tab, w_uq_t, w_uk, w_uv, w_out, hidden)


def solution(mesh):
    tp = mesh.shape["tp"]

    def local_step(hidden, lengths, rope_cos, rope_sin, cache_lat, cache_pe, norm_in, w_dq, norm_q, w_dkv, norm_kv, w_uq, w_uk, w_uv, w_out):
        seqs, tok, model = hidden.shape
        qlen = tok * tp
        kv_rank, heads, nope = w_uk.shape
        q_rank = w_dq.shape[1]
        rope = cache_pe.shape[2]
        cache_len = cache_lat.shape[1]
        prefix = cache_len - qlen
        me = lax.axis_index("tp")
        normed = rms_norm(hidden.astype(F32), norm_in).astype(BF16)
        q_latent = rms_norm(jnp.einsum("btd,dq->btq", normed, w_dq, preferred_element_type=F32), norm_q).astype(BF16)
        kv_proj = jnp.einsum("btd,dk->btk", normed, w_dkv, preferred_element_type=F32)
        new_lat = rms_norm(kv_proj[..., :kv_rank], norm_kv).astype(BF16)
        cos_own = lax.dynamic_slice_in_dim(rope_cos, me * tok, tok, axis=1)
        sin_own = lax.dynamic_slice_in_dim(rope_sin, me * tok, tok, axis=1)
        new_pe = apply_rope(kv_proj[..., kv_rank:], cos_own, sin_own).astype(BF16)
        packed = jnp.concatenate([q_latent, new_lat, new_pe, new_pe], axis=-1)
        gathered = lax.all_gather(packed, "tp", axis=1, tiled=True)
        lat_new = gathered[..., q_rank:q_rank + kv_rank]
        pe_new = gathered[..., q_rank + kv_rank:q_rank + kv_rank + rope]
        shift = jnp.arange(cache_len)[None, :] - lengths[:, None]
        pick = (shift[:, :, None] == jnp.arange(qlen)[None, None, :]).astype(BF16)
        inside = jnp.logical_and(shift >= 0, shift < qlen)[:, :, None]
        lat_all = jnp.where(inside, jnp.einsum("bti,bic->btc", pick, lat_new, preferred_element_type=F32).astype(BF16), cache_lat)
        pe_all = jnp.where(inside, jnp.einsum("bti,bic->btc", pick, pe_new, preferred_element_type=F32).astype(BF16), cache_pe)

        pe_old = jnp.concatenate([cache_pe[:, :prefix], cache_pe[:, :prefix]], axis=-1)
        cos_tab = jnp.concatenate([rope_cos] * 4, axis=-1)
        sin_tab = jnp.concatenate([-rope_sin, rope_sin] * 2, axis=-1)
        w_uq_t = jnp.transpose(w_uq, (1, 2, 0))
        block_out = attention_block(lengths, gathered, cache_lat, pe_old, cos_tab, sin_tab, w_uq_t,
                                    w_uk.reshape(kv_rank, heads * nope), w_uv.reshape(kv_rank, -1), w_out, hidden, tp)
        return block_out, lat_all, pe_all

    spec_tok = P("dp", "tp", None)
    spec_len = P("dp")
    spec_seq = P("dp", None, None)
    spec_vec = P(None)
    spec_mat = P(None, None)
    spec_head = P(None, "tp", None)
    spec_rows = P("tp", None)
    in_specs = (spec_tok, spec_len, spec_seq, spec_seq, spec_seq, spec_seq, spec_vec, spec_mat, spec_vec, spec_mat, spec_vec, spec_head, spec_head, spec_head, spec_rows)
    return jax.shard_map(local_step, mesh=mesh, in_specs=in_specs, out_specs=(spec_tok, spec_seq, spec_seq), check_vma=False)
```

```python
import functools
import types

import jax
import jax.numpy as jnp
from jax import lax
from jax.experimental import pallas as pl
from jax.experimental.pallas import tpu as pltpu
from jax.sharding import PartitionSpec as P

BF16 = jnp.bfloat16
F32 = jnp.float32
NEG = -1e30
LOG2E = 1.4426950408889634
EPS = 1e-6
QBLK = 128
CORES = 2
MAIN_ID = 0
PANEL = 256
RELAY_ROWS = 64
RELAY_SLOTS = 4


def rms_norm(values, gain_vec):
    mean_sq = jnp.sum(values * values, axis=-1, keepdims=True) * (1.0 / values.shape[-1])
    return values * lax.rsqrt(mean_sq + EPS) * gain_vec


def dot_nn(lhs, rhs):
    return lax.dot_general(lhs, rhs, (((1,), (0,)), ((), ())), preferred_element_type=F32)


def dot_nt(lhs, rhs):
    return lax.dot_general(lhs, rhs, (((1,), (1,)), ((), ())), preferred_element_type=F32)


def rope_pair(values, cos_tab, sin_tab, half_dim):
    lanes = values.shape[1]
    upper = pltpu.roll(values, lanes - half_dim, 1)
    lower = pltpu.roll(values, half_dim, 1)
    lane = lax.broadcasted_iota(jnp.int32, values.shape, 1)
    swapped = jnp.where(lane % (2 * half_dim) < half_dim, upper, lower)
    return values * cos_tab + swapped * sin_tab


KIND_PARTNER, KIND_LEFT, KIND_RIGHT, KIND_LEFT_PARTNER, KIND_RIGHT_PARTNER, KIND_LEFT_RIGHT, KIND_RIGHT_LEFT, KIND_FAR_A, KIND_FAR_B = range(9)
KINDS = 9
INPUTS = ("length", "hid", "cos", "sin", "lat", "pe", "g_in", "w_dq", "g_q", "w_dkv", "g_kv", "wuq", "wuk", "wuv", "wout")
OUTPUTS = ("out", "gath_q", "gath_kv")


def main_kernel(dm, names, *refs):
    r = types.SimpleNamespace(**dict(zip(names, refs, strict=True)))
    me = lax.axis_index("tp")
    chip = me // CORES
    core = me % CORES
    chips = dm.chips
    left_chip = (chip + chips - 1) % chips
    right_chip = (chip + 1) % chips
    far_chip = (chip + 2) % chips
    partner = chip * CORES + (1 - core)
    left = left_chip * CORES + core
    right = right_chip * CORES + core

    groups, gh = dm.groups, dm.group_heads
    chunks, cw, hw, tok = dm.chunks, dm.chunk_cols, dm.half_cols, dm.tok
    seqs = dm.seqs
    attn_ticks = seqs * groups
    out_ticks = seqs * chunks
    nope, rope, vdim, prefix, qlen = dm.nope, dm.rope, dm.vdim, dm.prefix, dm.qlen
    nslot = dm.ring_slots
    q_rank, kv_rank, model = dm.q_rank, dm.kv_rank, dm.model
    kv_cols = kv_rank + 2 * rope
    rows_own = seqs * tok

    def hidden_copy(b):
        return pltpu.make_async_copy(r.hid.at[b], r.act.at[pl.ds(b * tok, tok)], r.act_sem.at[b])

    def small_copies():
        return (
            pltpu.make_async_copy(r.g_in, r.gain_in.at[0], r.small_sem.at[0]),
            pltpu.make_async_copy(r.g_q, r.gain_q.at[0], r.small_sem.at[1]),
            pltpu.make_async_copy(r.g_kv, r.gain_kv.at[0], r.small_sem.at[2]),
            pltpu.make_async_copy(r.cos, r.cos_raw, r.small_sem.at[3]),
            pltpu.make_async_copy(r.sin, r.sin_raw, r.small_sem.at[4]),
        )

    def w_dkv_copies():
        return (
            pltpu.make_async_copy(r.w_dkv, r.wkv_down.at[pl.ds(0, kv_rank + rope)], r.wkv_sem.at[0]),
            pltpu.make_async_copy(r.w_dkv.at[pl.ds(kv_rank, rope)], r.wkv_down.at[pl.ds(kv_rank + rope, rope)], r.wkv_sem.at[1]),
        )

    def w_dq_copies(s):
        return tuple(
            pltpu.make_async_copy(r.w_dq.at[:, pl.ds((2 * s + p) * PANEL, PANEL)], r.wbuf.at[s % 2, pl.ds(p * model, model)], r.wbuf_sem.at[s % 2, p])
            for p in range(2)
        )

    def wout_copies(j):
        depth = r.wout.shape[0]
        return tuple(
            pltpu.make_async_copy(r.wout.at[:, pl.ds((j % chunks) * cw + p * PANEL, PANEL)], r.wbuf.at[j % 2, pl.ds(p * depth, depth)], r.wbuf_sem.at[j % 2, p])
            for p in range(cw // PANEL)
        )

    def relay_copy(src, n):
        slot = n % RELAY_SLOTS
        block = n % (kv_rank // RELAY_ROWS)
        return pltpu.make_async_copy(src.at[pl.ds(block * RELAY_ROWS, RELAY_ROWS)], r.relay.at[slot].reshape(RELAY_ROWS, dm.heads, nope), r.relay_sem.at[slot])

    def seq_copies(b):
        slot = b % 2
        return (
            pltpu.make_async_copy(r.gath_q.at[b], r.q_lat.at[slot], r.seq_sem.at[slot, 0]),
            pltpu.make_async_copy(r.lat.at[b, pl.ds(0, prefix)], r.lat_buf.at[slot, pl.ds(0, prefix)], r.seq_sem.at[slot, 1]),
            pltpu.make_async_copy(r.gath_kv.at[b, :, pl.ds(0, kv_rank)], r.lat_buf.at[slot, pl.ds(prefix, qlen)], r.seq_sem.at[slot, 2]),
            pltpu.make_async_copy(r.pe.at[b, :, pl.ds(0, prefix)], r.pe_old.at[slot], r.seq_sem.at[slot, 3]),
            pltpu.make_async_copy(r.gath_kv.at[b, :, pl.ds(kv_rank, 2 * rope)], r.pe_new.at[slot], r.seq_sem.at[slot, 4]),
        )

    def wuq_copies(i):
        g, slot = i % groups, i % 2
        return (
            pltpu.make_async_copy(r.wuq.at[pl.ds(g * gh, gh), pl.ds(0, nope)], r.wuq_buf.at[slot, pl.ds(0, gh * nope)].reshape(gh, nope, q_rank), r.wuq_sem.at[slot, 0]),
            pltpu.make_async_copy(r.wuq.at[pl.ds(g * gh, gh), pl.ds(nope, rope)], r.wuq_buf.at[slot, pl.ds(gh * nope, gh * rope)].reshape(gh, rope, q_rank), r.wuq_sem.at[slot, 1]),
        )

    def hid_copy(j):
        return pltpu.make_async_copy(r.hid.at[j // chunks, :, pl.ds((j % chunks) * cw, cw)], r.hid_buf.at[j % nslot], r.hid_sem.at[j % nslot])

    def y_copy(j):
        return pltpu.make_async_copy(r.y_buf.at[j % 2], r.out.at[j // chunks, :, pl.ds((j % chunks) * cw, cw)], r.y_sem.at[j % 2])

    half = tok // 2

    def gather_unit(b, is_q):
        dst = r.gath_q if is_q else r.gath_kv
        src = r.pack_q if is_q else r.pack_kv
        unit = b + (seqs if is_q else 0)

        def copy(kind, source, owner, offset, count, peer):
            rows = pl.ds(pl.multiple_of(owner * tok + offset, 8), count)
            return pltpu.make_async_remote_copy(
                src_ref=source if source is not None else dst.at[b, rows],
                dst_ref=dst.at[b, rows],
                send_sem=r.gath_send.at[unit, kind],
                recv_sem=r.gath_recv.at[unit, kind],
                device_id={"tp": peer},
            )

        far = far_chip * CORES + core
        return {
            KIND_PARTNER: lambda: copy(KIND_PARTNER, src.at[b], me, 0, tok, partner),
            KIND_LEFT: lambda: copy(KIND_LEFT, src.at[b], me, 0, tok, left),
            KIND_RIGHT: lambda: copy(KIND_RIGHT, src.at[b], me, 0, tok, right),
            KIND_LEFT_PARTNER: lambda: copy(KIND_LEFT_PARTNER, None, left, 0, tok, partner),
            KIND_RIGHT_PARTNER: lambda: copy(KIND_RIGHT_PARTNER, None, right, 0, tok, partner),
            KIND_LEFT_RIGHT: lambda: copy(KIND_LEFT_RIGHT, None, left, 0, half, right),
            KIND_RIGHT_LEFT: lambda: copy(KIND_RIGHT_LEFT, None, right, half, half, left),
            KIND_FAR_A: lambda: copy(KIND_FAR_A, None, far, 0, half, partner),
            KIND_FAR_B: lambda: copy(KIND_FAR_B, None, far, half, half, partner),
        }

    def local_copy(b, is_q):
        dst = r.gath_q if is_q else r.gath_kv
        src = r.pack_q if is_q else r.pack_kv
        unit = b + (seqs if is_q else 0)
        return pltpu.make_async_copy(src.at[b], dst.at[b, pl.ds(pl.multiple_of(me * tok, 8), tok)], r.local_sem.at[unit])

    scope = jax.named_scope

    def gather_send(b, is_q):
        copies = gather_unit(b, is_q)
        copies[KIND_LEFT]().start()
        copies[KIND_RIGHT]().start()
        copies[KIND_PARTNER]().start()
        local_copy(b, is_q).start()

    def gather_forward(b, is_q):
        copies = gather_unit(b, is_q)
        copies[KIND_RIGHT]().wait_recv()
        copies[KIND_LEFT_RIGHT]().start()
        copies[KIND_LEFT_PARTNER]().start()
        copies[KIND_LEFT]().wait_recv()
        copies[KIND_RIGHT_LEFT]().start()
        copies[KIND_RIGHT_PARTNER]().start()

    def gather_far(b, is_q):
        copies = gather_unit(b, is_q)
        copies[KIND_LEFT_RIGHT]().wait_recv()
        copies[KIND_FAR_A]().start()
        copies[KIND_RIGHT_LEFT]().wait_recv()
        copies[KIND_FAR_B]().start()

    def gather_done(b, is_q):
        copies = gather_unit(b, is_q)
        for kind in (KIND_PARTNER, KIND_LEFT_PARTNER, KIND_RIGHT_PARTNER, KIND_FAR_A, KIND_FAR_B):
            copies[kind]().wait_recv()
        local_copy(b, is_q).wait()

    def gather_drain(b, is_q):
        copies = gather_unit(b, is_q)
        for kind in range(KINDS):
            copies[kind]().wait_send()

    def xch_copy(j, t):
        slot = j % 2
        return pltpu.make_async_remote_copy(
            src_ref=r.part.at[pl.ds(pl.multiple_of((t * CORES + 1 - core) * tok, 8), tok), pl.ds(0, cw)],
            dst_ref=r.xch.at[slot, t],
            send_sem=r.xch_send.at[slot, t],
            recv_sem=r.xch_recv.at[slot, t],
            device_id={"tp": partner},
        )

    def toward(u):
        if u == 0:
            return left, left_chip, right, right_chip
        return right, right_chip, left, left_chip

    def ring_copy(name, j, u, block, peer):
        slot = j % nslot
        return pltpu.make_async_remote_copy(
            src_ref=r.sums.at[slot, block, :, pl.ds(u * hw, hw)],
            dst_ref=getattr(r, name).at[slot, u],
            send_sem=getattr(r, name + "_send").at[slot, u],
            recv_sem=getattr(r, name + "_recv").at[slot, u],
            device_id={"tp": peer},
        )

    def hop_copy(j, u):
        down, _, _, _ = toward(u)
        return ring_copy("hop", j, u, far_chip, down)

    def direct_copy(j, u):
        _, _, up, up_chip = toward(u)
        return ring_copy("direct", j, u, up_chip, up)

    def final_copy(j, u):
        down, down_chip, _, _ = toward(u)
        return ring_copy("final", j, u, down_chip, down)

    def attention(b, g, wslot):
        slot = b % 2
        q_lat = r.q_lat[slot]
        lane = lax.broadcasted_iota(jnp.int32, (qlen, 2 * rope), 1)
        q_pe = dot_nt(q_lat, r.wuq_buf[wslot, gh * nope:])
        for pair in range(gh // 2):
            rotated = rope_pair(q_pe[:, pair * 2 * rope:(pair + 1) * 2 * rope], r.cos_tab[b], r.sin_tab[b], rope // 2)
            r.qcat[2 * pair, :, nope:] = jnp.where(lane < rope, rotated, 0.0).astype(BF16)
            r.qcat[2 * pair + 1, :, nope:] = jnp.where(lane >= rope, rotated, 0.0).astype(BF16)
        q_nope = dot_nt(q_lat, r.wuq_buf[wslot, :gh * nope])
        for h in range(gh):
            r.qcat[h, :, :nope] = q_nope[:, h * nope:(h + 1) * nope].astype(BF16)
        keys = dot_nn(r.lat_buf[slot], r.wkv_up[0, g])
        for h in range(gh):
            r.kcat[h, :, :nope] = keys[:, h * nope:(h + 1) * nope].astype(BF16)
        r.vcat[...] = dot_nn(r.lat_buf[slot], r.wkv_up[1, g]).astype(BF16)

        key_pos = lax.broadcasted_iota(jnp.int32, (1, prefix), 1)
        bias = jnp.where(key_pos < r.length[b], 0.0, NEG).astype(F32)
        row = lax.broadcasted_iota(jnp.int32, (QBLK, QBLK), 0)
        col = lax.broadcasted_iota(jnp.int32, (QBLK, QBLK), 1)
        causal = col <= row
        nblk = qlen // QBLK
        wide = prefix + (nblk - 1) * QBLK
        for h in range(gh):
            main = dot_nt(r.qcat[h], r.kcat[h, :wide])
            last = dot_nt(r.qcat[h, (nblk - 1) * QBLK:], r.kcat[h, wide:])
            for blk in range(nblk):
                rows = slice(blk * QBLK, (blk + 1) * QBLK)
                pieces = [main[rows, :prefix] + bias]
                if blk == nblk - 1:
                    pieces.append(main[rows, prefix:wide])
                    diag = last
                else:
                    if blk > 0:
                        pieces.append(main[rows, prefix:prefix + blk * QBLK])
                    diag = main[rows, prefix + blk * QBLK:prefix + (blk + 1) * QBLK]
                pieces.append(jnp.where(causal, diag, NEG))
                top = functools.reduce(jnp.maximum, [jnp.max(piece, axis=1, keepdims=True) for piece in pieces])
                total = None
                acc = None
                start = 0
                for piece in pieces:
                    prob = jnp.exp2((piece - top) * dm.exp_scale)
                    piece_sum = jnp.sum(prob, axis=1, keepdims=True)
                    width = piece.shape[1]
                    term = dot_nn(prob.astype(BF16), r.vcat[start:start + width, h * vdim:(h + 1) * vdim])
                    total = piece_sum if total is None else total + piece_sum
                    acc = term if acc is None else acc + term
                    start += width
                r.attn[slot, rows, pl.ds(pl.multiple_of((g * gh + h) * vdim, 128), vdim)] = (acc / total).astype(BF16)

    for copy in small_copies():
        copy.start()
    for b in range(seqs):
        hidden_copy(b).start()
    for copy in w_dkv_copies():
        copy.start()

    barrier = pltpu.get_barrier_semaphore()
    for peer in (partner, left, right):
        pl.semaphore_signal(barrier, inc=1, device_id={"tp": peer})

    with scope("w_small"):
        for copy in small_copies():
            copy.wait()

    def rope_table(b, carry):
        cos_rows, sin_rows = r.cos_raw[b], r.sin_raw[b]
        r.cos_tab[b] = jnp.concatenate([cos_rows] * 4, axis=0).T
        r.sin_tab[b] = jnp.concatenate([-sin_rows, sin_rows] * 2, axis=0).T
        return carry

    for copy in w_dq_copies(0) + w_dq_copies(1):
        copy.start()

    with scope("rope_tab"):
        lax.fori_loop(0, seqs, rope_table, 0)

    norm_rows = 16

    def norm_step(n, carry):
        hidden_copy(n).wait()
        for part in range(tok // norm_rows):
            rows = pl.ds(pl.multiple_of(n * tok + part * norm_rows, norm_rows), norm_rows)
            r.act[rows] = rms_norm(r.act[rows].astype(F32), r.gain_in[...]).astype(BF16)
        return carry

    with scope("norm"):
        lax.fori_loop(0, seqs, norm_step, 0)

    with scope("w_dkv"):
        for copy in w_dkv_copies():
            copy.wait()
    with scope("dkv"):
        r.part[:rows_own, :kv_cols] = dot_nt(r.act[...], r.wkv_down[...])

    blocks = kv_rank // RELAY_ROWS
    for n in range(RELAY_SLOTS):
        relay_copy(r.wuk, n).start()
    for copy in wuq_copies(0):
        copy.start()

    with scope("w_barrier"):
        pl.semaphore_wait(barrier, 3)

    def kv_step(b, carry):
        rows = pl.ds(pl.multiple_of(b * tok, 16), tok)
        own = pl.ds(pl.multiple_of(me * tok, 16), tok)
        r.pack_kv[b, :, :kv_rank] = rms_norm(r.part[rows, :kv_rank], r.gain_kv[...]).astype(BF16)
        r.pack_kv[b, :, kv_rank:] = rope_pair(r.part[rows, kv_rank:kv_cols], r.cos_tab[b, own], r.sin_tab[b, own], rope // 2).astype(BF16)
        return carry

    lax.fori_loop(0, seqs, kv_step, 0)

    def kv_send(b, carry):
        gather_send(b, False)
        return carry

    with scope("kv_send"):
        lax.fori_loop(0, seqs, kv_send, 0)

    def dq_step(s, carry):
        for copy in w_dq_copies(s):
            copy.wait()
        act = r.act[...]
        for p in range(2):
            cols = pl.ds(pl.multiple_of((2 * s + p) * PANEL, PANEL), PANEL)
            r.part[:rows_own, cols] = dot_nn(act, r.wbuf[s % 2, p * model:(p + 1) * model])

        @pl.when(s + 2 < q_rank // (2 * PANEL))
        def _():
            for copy in w_dq_copies(s + 2):
                copy.start()

        return carry

    with scope("dq"):
        lax.fori_loop(0, q_rank // (2 * PANEL), dq_step, 0)

    def q_step(b, carry):
        rows = pl.ds(pl.multiple_of(b * tok, 16), tok)
        r.pack_q[b] = rms_norm(r.part[rows, :q_rank], r.gain_q[...]).astype(BF16)
        return carry

    lax.fori_loop(0, seqs, q_step, 0)

    with scope("send_q0"):
        gather_send(0, True)
        gather_forward(0, False)
        gather_send(1, True)

    def relay_step(n, carry):
        slot = n % RELAY_SLOTS
        relay_copy(r.wuk, n).wait()
        r.relay_f32[...] = r.relay[slot].astype(F32)

        @pl.when(n + RELAY_SLOTS < blocks)
        def _():
            relay_copy(r.wuk, n + RELAY_SLOTS).start()

        @pl.when(jnp.logical_and(n + RELAY_SLOTS >= blocks, n + RELAY_SLOTS < 2 * blocks))
        def _():
            relay_copy(r.wuv, n + RELAY_SLOTS).start()

        rows = pl.ds(pl.multiple_of((n % blocks) * RELAY_ROWS, RELAY_ROWS), RELAY_ROWS)
        for h in range(dm.heads):
            head_rows = r.relay_f32[pl.ds(h, RELAY_ROWS, stride=dm.heads), :]
            r.wkv_up[n // blocks, h // gh, rows, (h % gh) * nope:(h % gh + 1) * nope] = head_rows.astype(BF16)
        return carry

    with scope("relay"):
        lax.fori_loop(0, 2 * blocks, relay_step, 0)

    with scope("fwd_q0"):
        gather_forward(0, True)

    def kv_forward(b, carry):
        gather_forward(b, False)
        return carry

    with scope("kv_fwd"):
        gather_send(2, True)
        gather_send(3, True)
        lax.fori_loop(1, seqs, kv_forward, 0)
    with scope("far0"):
        gather_far(0, False)
        gather_far(0, True)
    with scope("done0"):
        gather_done(0, False)
        gather_done(0, True)
    for copy in seq_copies(0):
        copy.start()

    gather_plan = (
        (0, [(gather_forward, 1, True), (gather_send, 4, True)]),
        (1, [(gather_forward, 2, True), (gather_forward, 3, True), (gather_send, 5, True)]),
        (2, [(gather_far, 1, True)] + [(gather_far, v, False) for v in range(1, seqs)]),
        (3, [(gather_forward, 4, True)]),
        (4, [(gather_forward, 5, True), (gather_far, 2, True), (gather_far, 3, True)]),
        (5, [(gather_far, 4, True)]),
        (6, [(gather_far, 5, True)]),
    )

    def tick(i, carry):
        b = i // groups
        g = i % groups
        wslot = i % 2

        for at, steps in gather_plan:
            @pl.when(i == at)
            def _():
                with scope("t_gather"):
                    for step, seq, is_q in steps:
                        if seq < seqs:
                            step(seq, is_q)

        @pl.when(i + 1 < attn_ticks)
        def _():
            for copy in wuq_copies(i + 1):
                copy.start()

        @pl.when(jnp.logical_and(g == groups - 1, b + 1 < seqs))
        def _():
            with scope("t_done"):
                gather_done(b + 1, False)
                gather_done(b + 1, True)
            for copy in seq_copies(b + 1):
                copy.start()

        j_next = i + 1 - groups

        @pl.when(jnp.logical_and(j_next >= 0, j_next < out_ticks))
        def _():
            for copy in wout_copies(j_next):
                copy.start()

        j1 = i - groups - 1

        @pl.when(jnp.logical_and(j1 >= 0, j1 < out_ticks))
        def _():
            hid_copy(j1).start()
            with scope("w_xch"):
                for t in range(chips):
                    xch_copy(j1, t).wait_recv()
            for off in (2, 1, 3, 0):
                t = (chip + off) % chips
                rows = pl.ds(pl.multiple_of((t * CORES + core) * tok, 8), tok)
                r.sums[j1 % nslot, t] = r.part[rows, :cw] + r.xch[j1 % 2, t]

            @pl.when(j1 + 2 < out_ticks)
            def _():
                pl.semaphore_signal(r.credit_pair, inc=1, device_id={"tp": partner})

            @pl.when(j1 >= nslot)
            def _():
                with scope("w_credit"):
                    pl.semaphore_wait(r.credit_left, 1)
                    pl.semaphore_wait(r.credit_right, 1)

            for u in range(2):
                hop_copy(j1, u).start()
            for u in range(2):
                direct_copy(j1, u).start()

        j2 = i - groups - 2

        @pl.when(jnp.logical_and(j2 >= 0, j2 < out_ticks))
        def _():
            with scope("w_hop"):
                for u in range(2):
                    hop_copy(j2, u).wait_recv()
            for u in range(2):
                _, down_chip, _, _ = toward(u)
                cols = pl.ds(u * hw, hw)
                r.sums[j2 % nslot, down_chip, :, cols] = r.sums[j2 % nslot, down_chip, :, cols] + r.hop[j2 % nslot, u]
            for u in range(2):
                final_copy(j2, u).start()

        j3 = i - groups - 4

        @pl.when(jnp.logical_and(j3 >= 0, j3 < out_ticks))
        def _():
            s3 = j3 % nslot
            hid_copy(j3).wait()

            @pl.when(j3 >= 2)
            def _():
                y_copy(j3 - 2).wait()

            with scope("w_final"):
                for u in range(2):
                    direct_copy(j3, u).wait()
                    final_copy(j3, u).wait()
                    hop_copy(j3, u).wait_send()
            for u in range(2):
                cols = pl.ds(u * hw, hw)
                total = r.sums[s3, chip, :, cols] + r.direct[s3, u] + r.final[s3, u]
                r.y_buf[j3 % 2, :, cols] = (total + r.hid_buf[s3, :, cols].astype(F32)).astype(BF16)

            @pl.when(j3 + nslot < out_ticks)
            def _():
                pl.semaphore_signal(r.credit_left, inc=1, device_id={"tp": right})
                pl.semaphore_signal(r.credit_right, inc=1, device_id={"tp": left})

            y_copy(j3).start()

        j0 = i - groups

        @pl.when(jnp.logical_and(j0 >= 0, j0 < out_ticks))
        def _():
            @pl.when(j0 >= 1)
            def _():
                for t in range(chips):
                    xch_copy(j0 - 1, t).wait_send()

            with scope("w_wout"):
                for copy in wout_copies(j0):
                    copy.wait()
            with scope("project"):
                attn = r.attn[(j0 // chunks) % 2]
                depth = attn.shape[1]
                for p in range(cw // PANEL):
                    r.part[:, p * PANEL:(p + 1) * PANEL] = dot_nn(attn, r.wbuf[j0 % 2, p * depth:(p + 1) * depth])

            @pl.when(j0 >= 2)
            def _():
                pl.semaphore_wait(r.credit_pair, 1)

            for t in range(chips):
                xch_copy(j0, t).start()

        @pl.when(i < attn_ticks)
        def _():
            @pl.when(g == 0)
            def _():
                with scope("w_seq"):
                    for copy in seq_copies(b):
                        copy.wait()
                old_rows = r.pe_old[b % 2].astype(F32)
                old_pe = jnp.concatenate([old_rows, old_rows], axis=0).T.astype(BF16)
                for h in range(gh):
                    r.kcat[h, :prefix, nope:] = old_pe
                    r.kcat[h, prefix:, nope:] = r.pe_new[b % 2]

            with scope("w_wuq"):
                for copy in wuq_copies(i):
                    copy.wait()
            with scope("attend"):
                attention(b, g, wslot)

        return carry

    lax.fori_loop(0, out_ticks + groups + 4, tick, 0)

    for t in range(chips):
        xch_copy(out_ticks - 1, t).wait_send()
    for j in (out_ticks - 2, out_ticks - 1):
        y_copy(j).wait()

    def drain(b, carry):
        gather_drain(b, False)
        gather_drain(b, True)
        return carry

    lax.fori_loop(0, seqs, drain, 0)


def attention_block(tp, length, hid, cos, sin, lat, pe, g_in, w_dq, g_q, w_dkv, g_kv, wuq, wuk, wuv, wout):
    dm = types.SimpleNamespace()
    dm.seqs, dm.tok, dm.model = hid.shape
    dm.heads, head_dim, dm.q_rank = wuq.shape
    dm.kv_rank, _, dm.nope = wuk.shape
    dm.vdim = wuv.shape[2]
    dm.rope = head_dim - dm.nope
    dm.qlen = dm.tok * tp
    dm.prefix = lat.shape[1] - dm.qlen
    dm.chips = tp // CORES
    dm.group_heads = 4
    dm.groups = dm.heads // dm.group_heads
    dm.chunks = 4
    dm.chunk_cols = dm.model // dm.chunks
    dm.half_cols = dm.chunk_cols // 2
    dm.ring_slots = 4
    dm.exp_scale = head_dim ** -0.5 * LOG2E
    gh, keys, ns, kv_cols = dm.group_heads, dm.prefix + dm.qlen, dm.ring_slots, dm.kv_rank + 2 * dm.rope
    assert dm.chips == 4 and dm.groups == dm.chunks and dm.vdim == dm.nope

    def vmem(*shape, dtype=BF16):
        return pltpu.VMEM(shape, dtype)

    def dma(*shape):
        return pltpu.SemaphoreType.DMA(shape)

    wbuf_rows = max(2 * dm.model, (dm.chunk_cols // PANEL) * dm.heads * dm.vdim)
    part_cols = max(dm.chunk_cols, dm.q_rank)
    ring = (ns, 2, dm.tok, dm.half_cols)
    credit = pltpu.SemaphoreType.REGULAR
    scratch = dict(
        act=vmem(dm.seqs * dm.tok, dm.model),
        gain_in=vmem(1, dm.model, dtype=F32), gain_q=vmem(1, dm.q_rank, dtype=F32), gain_kv=vmem(1, dm.kv_rank, dtype=F32),
        cos_raw=vmem(*cos.shape, dtype=F32), sin_raw=vmem(*cos.shape, dtype=F32),
        cos_tab=vmem(dm.seqs, dm.qlen, 2 * dm.rope, dtype=F32), sin_tab=vmem(dm.seqs, dm.qlen, 2 * dm.rope, dtype=F32),
        wkv_down=vmem(kv_cols, dm.model),
        wbuf=vmem(2, wbuf_rows, PANEL),
        part=vmem(dm.qlen, part_cols, dtype=F32),
        pack_q=vmem(dm.seqs, dm.tok, dm.q_rank), pack_kv=vmem(dm.seqs, dm.tok, kv_cols),
        relay=vmem(RELAY_SLOTS, RELAY_ROWS * dm.heads, dm.nope), relay_f32=vmem(RELAY_ROWS * dm.heads, dm.nope, dtype=F32),
        wkv_up=vmem(2, dm.groups, dm.kv_rank, gh * dm.nope),
        q_lat=vmem(2, dm.qlen, dm.q_rank),
        lat_buf=vmem(2, keys, dm.kv_rank),
        pe_old=vmem(2, dm.rope, dm.prefix), pe_new=vmem(2, dm.qlen, 2 * dm.rope),
        wuq_buf=vmem(2, gh * head_dim, dm.q_rank),
        qcat=vmem(gh, dm.qlen, dm.nope + 2 * dm.rope), kcat=vmem(gh, keys, dm.nope + 2 * dm.rope), vcat=vmem(keys, gh * dm.vdim),
        attn=vmem(2, dm.qlen, dm.heads * dm.vdim),
        xch=vmem(2, dm.chips, dm.tok, dm.chunk_cols, dtype=F32),
        sums=vmem(ns, dm.chips, dm.tok, dm.chunk_cols, dtype=F32),
        hop=vmem(*ring, dtype=F32), direct=vmem(*ring, dtype=F32), final=vmem(*ring, dtype=F32),
        hid_buf=vmem(ns, dm.tok, dm.chunk_cols), y_buf=vmem(2, dm.tok, dm.chunk_cols),
        act_sem=dma(dm.seqs), small_sem=dma(5), wkv_sem=dma(2), wbuf_sem=dma(2, max(2, dm.chunk_cols // PANEL)), relay_sem=dma(RELAY_SLOTS),
        seq_sem=dma(2, 5), wuq_sem=dma(2, 2), hid_sem=dma(ns), y_sem=dma(2),
        local_sem=dma(2 * dm.seqs), gath_send=dma(2 * dm.seqs, KINDS), gath_recv=dma(2 * dm.seqs, KINDS),
        xch_send=dma(2, dm.chips), xch_recv=dma(2, dm.chips),
        hop_send=dma(ns, 2), hop_recv=dma(ns, 2), direct_send=dma(ns, 2), direct_recv=dma(ns, 2), final_send=dma(ns, 2), final_recv=dma(ns, 2),
        credit_pair=credit, credit_left=credit, credit_right=credit,
    )
    hbm = pl.BlockSpec(memory_space=pl.ANY)
    block_out, _, gath_kv = pl.pallas_call(
        functools.partial(main_kernel, dm, INPUTS + OUTPUTS + tuple(scratch)),
        out_shape=(
            jax.ShapeDtypeStruct(hid.shape, BF16),
            jax.ShapeDtypeStruct((dm.seqs, dm.qlen, dm.q_rank), BF16),
            jax.ShapeDtypeStruct((dm.seqs, dm.qlen, kv_cols), BF16),
        ),
        in_specs=[pl.BlockSpec(memory_space=pltpu.SMEM)] + [hbm] * (len(INPUTS) - 1),
        out_specs=(hbm, hbm, hbm),
        scratch_shapes=list(scratch.values()),
        compiler_params=pltpu.CompilerParams(collective_id=MAIN_ID, has_side_effects=True, vmem_limit_bytes=67_000_000),
        name="attend_project",
    )(length, hid, cos, sin, lat, pe, g_in, w_dq, g_q, w_dkv, g_kv, wuq, wuk, wuv, wout)
    return block_out, gath_kv


def cache_kernel(kv_rank, len_ref, lat_ref, pe_ref, new_ref, y_ref, lat_out, pe_out, y_out):
    length = len_ref[pl.program_id(0)]
    rows, count = lat_ref.shape[1], new_ref.shape[1]
    rope = pe_ref.shape[1]
    pick = lax.broadcasted_iota(jnp.int32, (rows, count), 0) - lax.broadcasted_iota(jnp.int32, (rows, count), 1) == length
    picked = dot_nn(pick.astype(F32).astype(BF16), new_ref[0])
    shift = lax.broadcasted_iota(jnp.int32, (rows, kv_rank), 0) - length
    lat_out[0] = jnp.where(jnp.logical_and(shift >= 0, shift < count), picked[:, :kv_rank], lat_ref[0].astype(F32)).astype(BF16)
    picked_pe = picked[:, kv_rank:].T[:rope]
    shift = lax.broadcasted_iota(jnp.int32, (rope, rows), 1) - length
    pe_out[0] = jnp.where(jnp.logical_and(shift >= 0, shift < count), picked_pe, pe_ref[0].astype(F32)).astype(BF16)
    y_out[...] = y_ref[...]


def update_caches(length, lat, pe, gath_kv, block_out):
    def spec(shape):
        return pl.BlockSpec((1,) + shape[1:], lambda b, length: (b, 0, 0))

    shapes = [lat.shape, pe.shape, gath_kv.shape, block_out.shape]
    return pl.pallas_call(
        functools.partial(cache_kernel, lat.shape[2]),
        out_shape=tuple(jax.ShapeDtypeStruct(shape, BF16) for shape in (lat.shape, pe.shape, block_out.shape)),
        grid_spec=pltpu.PrefetchScalarGridSpec(
            num_scalar_prefetch=1, grid=(lat.shape[0],),
            in_specs=[spec(shape) for shape in shapes],
            out_specs=[spec(shape) for shape in (lat.shape, pe.shape, block_out.shape)],
        ),
        compiler_params=pltpu.CompilerParams(vmem_limit_bytes=67_000_000),
        name="write_caches",
    )(length, lat, pe, gath_kv, block_out)


def solution(mesh):
    tp = mesh.shape["tp"]

    def local_step(hidden, lengths, rope_cos, rope_sin, cache_lat, cache_pe, norm_in, w_dq, norm_q, w_dkv, norm_kv, w_uq, w_uk, w_uv, w_out):
        pe_t = jnp.transpose(cache_pe, (0, 2, 1))
        block_out, gath_kv = attention_block(
            tp, lengths, hidden, jnp.transpose(rope_cos, (0, 2, 1)), jnp.transpose(rope_sin, (0, 2, 1)), cache_lat, pe_t,
            norm_in, w_dq, norm_q, w_dkv.T, norm_kv, jnp.transpose(w_uq, (1, 2, 0)), w_uk, w_uv, w_out)
        lat_all, pe_all_t, block_out = update_caches(lengths, cache_lat, pe_t, gath_kv, block_out)
        return block_out, lat_all, jnp.transpose(pe_all_t, (0, 2, 1))

    spec_tok = P("dp", "tp", None)
    spec_len = P("dp")
    spec_seq = P("dp", None, None)
    spec_vec = P(None)
    spec_mat = P(None, None)
    spec_head = P(None, "tp", None)
    spec_rows = P("tp", None)
    in_specs = (spec_tok, spec_len, spec_seq, spec_seq, spec_seq, spec_seq, spec_vec, spec_mat, spec_vec, spec_mat, spec_vec, spec_head, spec_head, spec_head, spec_rows)
    return jax.shard_map(local_step, mesh=mesh, in_specs=in_specs, out_specs=(spec_tok, spec_seq, spec_seq), check_vma=False)
```
